32 devices in a mesh: groups: 2 (over x), ctx: 16 (over z, y, core).
Axes of the slice: x: 2, y: 2, z: 4, core: 2. Of those that a mesh axis runs over, the one named last changes fastest.
Arguments:
- queries: bfloat16 [3072, 16, 128], P(('groups', 'ctx')), parts along dimension 0, may hold values from -12 to 12
- keys: bfloat16 [3072, 4, 128], P(('groups', 'ctx')), parts along dimension 0, may hold values from -5 to 5
- values: bfloat16 [3072, 4, 128], P(('groups', 'ctx')), parts along dimension 0, may hold values from -6 to 6
- positions: int32 [3072], P(('groups', 'ctx')), parts along dimension 0, may hold values from 0 to 1535, as said below
Outputs:
- attended: bfloat16 [3072, 16, 128], P(('groups', 'ctx')), parts along dimension 0
The draws below stay inside these ranges and needn't reach their ends.
There are 2 independent parts, one for each index of `groups`. The reference program is written for one: setup_inputs(seed, part) draws one part's arguments, and reference() takes and returns one part's arrays. A program takes and returns all parts, laid end to end along the dimension named above; each array names one. Nothing has to cross between parts.
Inputs may be any that keep to these rules, and one draw needn't show every extreme that they name: A permutation of 0 to 1535 in which the 96 rows of each device along ctx hold the positions c, c + 16, c + 32 and so on in that order, for one offset c a device, the offsets of the devices being a permutation of 0 to 15.
All inputs are finite; a program needn't handle non-finite values.
Results may differ from the reference program's by a relative error of at most 0.0091.
Values may be sent and summed in bfloat16 or wider, within the bound.
A program may use at most 64 MiB of HBM per device.

```python
import math
import jax
import jax.numpy as jnp
from jax import lax

H = 16
KVH = 4
HD = 128
TOK_DEV = 96
SEQ = 1536
STRIDE = 16


def draw_common(key):
    base = jax.random.fold_in(key, 11)
    first_key, second_key = jax.random.split(base, 2)
    query_draw = jnp.clip(jax.random.normal(first_key, (SEQ, H, HD), jnp.float32) * 2.5, -12.0, 12.0)
    key_draw = jnp.clip(jax.random.normal(second_key, (SEQ, KVH, HD), jnp.float32), -5.0, 5.0)
    return (query_draw, key_draw)


def draw_queries(key, part):
    return draw_common(key)[0].astype(jnp.bfloat16)


def draw_keys(key, part):
    return draw_common(key)[1].astype(jnp.bfloat16)


def draw_positions(key, part):
    offsets = jax.random.permutation(jax.random.fold_in(key, 3), STRIDE)
    steps_along = jnp.arange(TOK_DEV, dtype=jnp.int32)
    placed = steps_along[None, :] * STRIDE + offsets.astype(jnp.int32)[:, None]
    return placed.reshape(-1).astype(jnp.int32)


def levels(stream_key, dims, pieces, low, largest):
    factor_of, own = 1.0, jax.random.fold_in(stream_key, 6)
    for dim, blocks in pieces:
        steps = jnp.exp(jax.random.uniform(jax.random.fold_in(own, dim), (blocks,), jnp.float32, low / len(pieces), largest / len(pieces)))
        factor_of = factor_of * jnp.repeat(steps, dims[dim] // blocks).reshape([-1 if axis == dim else 1 for axis in range(len(dims))])
    return factor_of


def scatter_about(stream_key, extent, width, limit, cuts=(), kind=jnp.bfloat16):
    drawn = width * jax.random.normal(stream_key, extent, jnp.float32)
    if cuts:
        drawn = drawn * levels(stream_key, extent, cuts, -0.22, 0.18)
    return jnp.clip(drawn, -limit, limit).astype(kind)


def setup_inputs(seed: int = 0, part: int = 0) -> dict:
    key_of = jax.random.split(jax.random.key(seed), 5)
    part_splits = jax.random.split(jax.random.fold_in(key_of[4], part), 5)
    return {
        "queries": draw_queries(jax.random.fold_in(jax.random.fold_in(key_of[4], part), 71), part),
        "keys": draw_keys(jax.random.fold_in(jax.random.fold_in(key_of[4], part), 71), part),
        "values": scatter_about(part_splits[2], (SEQ, KVH, HD), 1.0, 6.0, ((0, 16),)),
        "positions": draw_positions(jax.random.fold_in(jax.random.fold_in(key_of[4], part), 71), part),
    }


def rotate(tensor, places):
    half_size = tensor.shape[-1] // 2
    inverse = jnp.power(jnp.float32(1000000.0), -jnp.arange(half_size, dtype=jnp.float32) * 2.0 / tensor.shape[-1])
    angles = places.astype(jnp.float32)[:, None] * inverse[None, :]
    cosine = jnp.cos(angles)[:, None, :]
    sines = jnp.sin(angles)[:, None, :]
    floats = tensor.astype(jnp.float32)
    leading = floats[..., :half_size]
    trailing = floats[..., half_size:]
    return jnp.concatenate([leading * cosine - trailing * sines, trailing * cosine + leading * sines], -1).astype(jnp.bfloat16)

def reference(queries, keys, values, positions):
    q_rot = rotate(queries, positions)
    k_rot = rotate(keys, positions)
    scaling = 1.0 / math.sqrt(HD)
    rows_block = math.gcd(SEQ, 512)
    grouped = q_rot.reshape(SEQ // rows_block, rows_block, KVH, H // KVH, HD)
    places = positions.reshape(SEQ // rows_block, rows_block)
    key_float = k_rot.astype(jnp.float32)
    value_float = values.astype(jnp.float32)

    def one_block(inputs):
        query_part, query_places = inputs
        scores = jnp.einsum('bkgd,skd->kgbs', query_part.astype(jnp.float32), key_float) * scaling
        allowed = query_places[:, None] >= positions[None, :]
        scores = jnp.where(allowed[None, None], scores, -jnp.inf)
        maxima = lax.optimization_barrier(jnp.max(scores, axis=-1, keepdims=True))
        weights = jnp.exp(scores - maxima)
        totals = lax.optimization_barrier(jnp.sum(weights, axis=-1))
        rounded = lax.optimization_barrier(weights.astype(jnp.bfloat16)).astype(jnp.float32)
        output = jnp.einsum('kgbs,skd->kgbd', rounded, value_float) / totals[..., None]
        return output.transpose(2, 0, 1, 3).reshape(rows_block, H, HD).astype(jnp.bfloat16)
    outputs = lax.map(one_block, (grouped, places))
    return outputs.reshape(SEQ, H, HD)
```

```python
import functools
import math

import jax
import jax.numpy as jnp
import numpy as np
from jax import lax
from jax.experimental import pallas as pl
from jax.experimental.pallas import tpu as pltpu
from jax.sharding import PartitionSpec as P

TILE = 32
DOWN, UP = 0, 1


def rotary_tables(tokens, head_size, stride):
    half = head_size // 2
    inverse = 1000000.0 ** (-2.0 * np.arange(half) / head_size)
    wide = lambda x: np.concatenate([x, x], -1)
    steps = (stride * np.arange(tokens))[:, None] * inverse[None, :]
    starts = np.arange(stride)[:, None] * inverse[None, :]
    return np.concatenate(
        [wide(np.cos(steps)), wide(np.sin(steps)), wide(np.cos(starts)), wide(np.sin(starts))]
    ).astype(np.float32)


def attend(
    n, kv_heads, per_group, tokens,
    place_hbm, q_hbm, k_hbm, v_hbm, table_hbm, out_ref,
    kv, kv_stage, q_all, q_stage, o_all, o_stage, offs, wide, small, m_ref, l_ref, acc_ref,
    place_ref, q_ref, k_ref, v_ref, table_ref,
    kv_recv, z_send, off_recv, offz_send, in_recv, in_send, inoff_recv, inoff_send,
    q_recv, q_send, o_recv, o_send, load_sem,
):
    loads = [
        pltpu.make_async_copy(src, dst, load_sem.at[i])
        for i, (src, dst) in enumerate(
            [(place_hbm, place_ref), (table_hbm, table_ref), (k_hbm, k_ref), (v_hbm, v_ref), (q_hbm, q_ref)]
        )
    ]
    for load in loads:
        load.start()
    head_size = q_ref.shape[-1]
    heads = kv_heads * per_group
    quartet = kv_heads
    rows = n // quartet
    pieces = tokens // TILE
    lanes = 2 * per_group * TILE
    factor = math.log2(math.e) / math.sqrt(head_size)
    me = lax.axis_index("ctx")
    z = me // quartet
    h = me % quartet
    column = h // 2
    core = h % 2
    mate = column * 2 + 1 - core
    across = (1 - column) * 2 + core
    diagonal = (1 - column) * 2 + 1 - core
    base = z * quartet
    targets = (me - quartet, me + quartet)
    onward = (z > 0, z < rows - 1)

    barrier = pltpu.get_barrier_semaphore()

    def greet(target):
        pl.semaphore_signal(barrier, inc=1, device_id={"ctx": target})

    for peer in (mate, across, diagonal):
        greet(base + peer)
    for way in (DOWN, UP):

        @pl.when(onward[way])
        def _():
            greet(targets[way])

    def remote(src, dst, send_sem, recv_sem, target):
        return pltpu.make_async_remote_copy(
            src_ref=src, dst_ref=dst, send_sem=send_sem, recv_sem=recv_sem, device_id={"ctx": target}
        )

    def piece(way, row, p, half, first=None, count=2):
        first = 2 * half if first is None else first
        part = kv.at[row, p, pl.ds(first, count)]
        return remote(part, part, z_send.at[way, row, p, half], kv_recv.at[row, p, half], targets[way])

    def mark(way, row, first=0, count=quartet):
        part = offs.at[row, pl.ds(first, count)]
        return remote(part, part, offz_send.at[way, row], off_recv.at[row], targets[way])

    def near(p, src, dst):
        return remote(kv_stage.at[dst, p], kv.at[z, p, src], in_send.at[p, dst], in_recv.at[p, src], base + dst)

    def near_mark(src, dst):
        part = offs.at[z, src]
        return remote(part, part, inoff_send.at[dst], inoff_recv.at[src], base + dst)

    def near_q(src, dst):
        return remote(
            q_stage.at[dst], q_all.at[src // 2, :, src % 2], q_send.at[dst], q_recv.at[src], base + dst
        )

    def back(p, src, dst):
        return remote(o_stage.at[p, dst], o_all.at[p, src], o_send.at[p, dst], o_recv.at[p, src], base + dst)

    for load in loads[:2]:
        load.wait()
    offset = place_ref[0]
    c0 = table_ref[pl.ds(2 * tokens + offset, 1), :]
    s0 = table_ref[pl.ds(2 * tokens + n + offset, 1), :]
    ct, st = table_ref[:tokens, :], table_ref[tokens : 2 * tokens, :]
    lane = lax.broadcasted_iota(jnp.int32, (tokens, head_size), 1)
    cosine = ct * c0 - st * s0
    sine = st * c0 + ct * s0
    sine = jnp.where(lane < head_size // 2, -sine, sine)

    def rotated(x):
        return (x * cosine + pltpu.roll(x, head_size // 2, 1) * sine).astype(jnp.bfloat16)

    offs[z, h] = jnp.full((1, head_size), offset.astype(jnp.float32), jnp.float32)
    for load in loads[2:4]:
        load.wait()
    small[0] = k_ref[...].astype(jnp.float32)
    small[1] = v_ref[...].astype(jnp.float32)
    for k in range(kv_heads):
        x = rotated(small[0, pl.ds(k, tokens, stride=kv_heads), :])
        kv_stage[k, :, 0] = x.reshape(pieces, TILE, head_size)
        x = small[1, pl.ds(k, tokens, stride=kv_heads), :].astype(jnp.bfloat16)
        kv_stage[k, :, 1] = x.reshape(pieces, TILE, head_size)
    for p in range(pieces):
        kv[z, p, h] = kv_stage[h, p]

    pl.semaphore_wait(barrier, 3 + onward[DOWN].astype(jnp.int32) + onward[UP].astype(jnp.int32))

    def spread(src):
        for way in (DOWN, UP):

            @pl.when(onward[way])
            def _():
                mark(way, z, src, 1).start()
                for p in range(pieces):
                    piece(way, z, p, src // 2, src, 1).start()

    for dst in (across, diagonal, mate):
        near_mark(h, dst).start()
    for p in range(pieces):
        for dst in (across, diagonal, mate):
            near(p, h, dst).start()
    spread(h)

    loads[4].wait()
    wide[...] = q_ref[...].astype(jnp.float32)
    for k in range(kv_heads):
        for g in range(per_group):
            q = rotated(wide[pl.ds(k * per_group + g, tokens, stride=heads), :])
            q_stage[k, :, g] = q.reshape(pieces, TILE, head_size)
    for dst in (across, diagonal, mate):
        near_q(h, dst).start()
    q_all[column, :, core] = q_stage[h]

    near_mark(mate, h).wait_recv()
    for p in range(pieces):
        near(p, mate, h).wait_recv()
    spread(mate)

    m_ref[...] = jnp.full(m_ref.shape, -jnp.inf, jnp.float32)
    l_ref[...] = jnp.zeros(l_ref.shape, jnp.float32)
    acc_ref[...] = jnp.zeros(acc_ref.shape, jnp.float32)

    for src in (across, diagonal):
        near_mark(src, h).wait_recv()
        for way in (DOWN, UP):

            @pl.when(onward[way])
            def _():
                mark(way, z, src, 1).start()

    for p in range(pieces):
        for src in (across, diagonal):
            near(p, src, h).wait_recv()
            for way in (DOWN, UP):

                @pl.when(onward[way])
                def _():
                    piece(way, z, p, src // 2, src, 1).start()

    keys_tile = quartet * TILE
    key_at = (lax.broadcasted_iota(jnp.int32, (keys_tile, lanes), 0) % TILE * n).astype(jnp.float32)
    query_at = (lax.broadcasted_iota(jnp.int32, (1, lanes), 1) % TILE * n).astype(jnp.float32)

    def attention(col, row, p):
        keys = kv[row, p, :, 0].reshape(keys_tile, head_size)
        values = kv[row, p, :, 1].reshape(keys_tile, head_size)
        first = p * lanes
        q = q_all[col, p:].reshape((pieces - p) * lanes, head_size)
        s = lax.dot_general(keys, q, (((1,), (1,)), ((), ())), preferred_element_type=jnp.float32)
        theirs = jnp.concatenate(
            [jnp.broadcast_to(jnp.concatenate([offs[row, i]] * (lanes // head_size), 1), (TILE, lanes)) for i in range(quartet)], 0
        )
        ours = jnp.concatenate(
            [jnp.concatenate([offs[z, 2 * col + i]] * (lanes // 2 // head_size), 1) for i in range(2)], 1
        )
        allowed = key_at + theirs <= query_at + ours
        head = jnp.where(allowed, s[:, :lanes], -jnp.inf)
        s = jnp.concatenate([head, s[:, lanes:]], 1) if p < pieces - 1 else head
        old = m_ref[col, :, first:]
        top = jnp.maximum(old, jnp.max(s, axis=0, keepdims=True))
        shrink = jnp.exp2((old - top) * factor)
        w = jnp.exp2((s - top) * factor)
        m_ref[col, :, first:] = top
        l_ref[col, :, first:] = l_ref[col, :, first:] * shrink + jnp.sum(w, axis=0, keepdims=True)
        o = lax.dot_general(
            values, w.astype(jnp.bfloat16), (((0,), (0,)), ((), ())), preferred_element_type=jnp.float32
        )
        acc_ref[col, :, first:] = acc_ref[col, :, first:] * shrink + o

    def events(k):
        return [(k - p, p) for p in reversed(range(pieces))]

    def each(k, do):
        for d, p in events(k):
            if isinstance(d, int) and not 1 <= d < rows:
                continue
            for way in (DOWN, UP):
                row = z + d if way == DOWN else z - d
                here = (row < rows) if way == DOWN else (row >= 0)
                if not isinstance(d, int):
                    here = here & (d >= 1) & (d < rows)

                @pl.when(here)
                def _():
                    do(way, row, p)

    def relay(k):
        def do(way, row, p):
            @pl.when(onward[way])
            def _():
                if p == 0:
                    mark(way, row).wait_recv()
                    mark(way, row).start()
                for half in (column, 1 - column):
                    piece(way, row, p, half).wait_recv()
                    piece(way, row, p, half).start()

        each(k, do)

    def take(k, cols, wait=True):
        def do(way, row, p):
            if wait:

                @pl.when(jnp.logical_not(onward[way]))
                def _():
                    if p == 0:
                        mark(way, row).wait_recv()
                    for half in (column, 1 - column):
                        piece(way, row, p, half).wait_recv()

            for col in cols:
                attention(col, row, p)

        each(k, do)

    def finish(p):
        for col in range(2):
            o = acc_ref[col, :, p * lanes : (p + 1) * lanes] / l_ref[col, :, p * lanes : (p + 1) * lanes]
            o = o.T.astype(jnp.bfloat16)
            for c in range(2):
                part = o[c * lanes // 2 : (c + 1) * lanes // 2]
                o_stage[p, 2 * col + c] = part.reshape(per_group, TILE, head_size)
        for dst in (across, diagonal, mate):
            back(p, h, dst).start()
        o_all[p, h] = o_stage[p, h]

    relay(1)
    for p in range(pieces):
        if p == 0:
            near_q(mate, h).wait_recv()
        attention(column, z, p)
    relay(2)
    take(1, [column])
    for src in (across, diagonal):
        near_q(src, h).wait_recv()
    for p in range(pieces):
        attention(1 - column, z, p)
    take(1, [1 - column], wait=False)

    @pl.loop(2, rows)
    def _(k):
        relay(k + 1)
        take(k, [0, 1])

    finish(0)
    for p in range(1, pieces):
        k = rows - 1 + p
        if p < pieces - 1:
            relay(k + 1)
        take(k, [0, 1])
        finish(p)

    for p in range(pieces):
        for src in (across, diagonal, mate):
            back(p, src, h).wait_recv()
        for k in range(kv_heads):
            for g in range(per_group):
                at = p * TILE * heads + k * per_group + g
                wide[pl.ds(at, TILE, stride=heads), :] = o_all[p, k, g].astype(jnp.float32)
        span = slice(p * TILE * heads, (p + 1) * TILE * heads)
        out_ref[span, :] = wide[span, :].astype(jnp.bfloat16)

    for dst in (across, diagonal, mate):
        near_mark(h, dst).wait_send()
        near_q(h, dst).wait_send()
        for p in range(pieces):
            near(p, h, dst).wait_send()
            back(p, h, dst).wait_send()

    def sent(way, row):
        @pl.when(onward[way])
        def _():
            mark(way, row).wait_send()
            for p in range(pieces):
                for half in range(2):
                    piece(way, row, p, half).wait_send()

    for way in (DOWN, UP):
        sent(way, z)

    @pl.loop(1, rows)
    def _(d):
        @pl.when(z + d < rows)
        def _():
            sent(DOWN, z + d)

        @pl.when(z - d >= 0)
        def _():
            sent(UP, z - d)


def solution(mesh):
    n = mesh.shape["ctx"]

    def shards(queries, keys, values, positions):
        tokens, heads, head_size = queries.shape
        kv_heads = keys.shape[1]
        per_group = heads // kv_heads
        table = rotary_tables(tokens, head_size, n)
        pieces = tokens // TILE
        rows = n // kv_heads
        width = 2 * per_group * tokens
        vmem = pl.BlockSpec(memory_space=pltpu.VMEM)
        hbm = pl.BlockSpec(memory_space=pl.ANY)
        dma = pltpu.SemaphoreType.DMA
        bf16, f32 = jnp.bfloat16, jnp.float32
        out = pl.pallas_call(
            functools.partial(attend, n, kv_heads, per_group, tokens),
            out_shape=jax.ShapeDtypeStruct((tokens * heads, head_size), bf16),
            in_specs=[hbm] * 5,
            out_specs=vmem,
            scratch_shapes=[
                pltpu.VMEM((rows, pieces, kv_heads, 2, TILE, head_size), bf16),
                pltpu.VMEM((kv_heads, pieces, 2, TILE, head_size), bf16),
                pltpu.VMEM((2, pieces, 2, per_group, TILE, head_size), bf16),
                pltpu.VMEM((kv_heads, pieces, per_group, TILE, head_size), bf16),
                pltpu.VMEM((pieces, kv_heads, per_group, TILE, head_size), bf16),
                pltpu.VMEM((pieces, kv_heads, per_group, TILE, head_size), bf16),
                pltpu.VMEM((rows, kv_heads, 1, head_size), f32),
                pltpu.VMEM((tokens * heads, head_size), f32),
                pltpu.VMEM((2, tokens * kv_heads, head_size), f32),
                pltpu.VMEM((2, 1, width), f32),
                pltpu.VMEM((2, 1, width), f32),
                pltpu.VMEM((2, head_size, width), f32),
                pltpu.SMEM((tokens,), jnp.int32),
                pltpu.VMEM((tokens * heads, head_size), bf16),
                pltpu.VMEM((tokens * kv_heads, head_size), bf16),
                pltpu.VMEM((tokens * kv_heads, head_size), bf16),
                pltpu.VMEM(table.shape, f32),
                dma((rows, pieces, 2)),
                dma((2, rows, pieces, 2)),
                dma((rows,)),
                dma((2, rows)),
                dma((pieces, kv_heads)),
                dma((pieces, kv_heads)),
                dma((kv_heads,)),
                dma((kv_heads,)),
                dma((kv_heads,)),
                dma((kv_heads,)),
                dma((pieces, kv_heads)),
                dma((pieces, kv_heads)),
                dma((5,)),
            ],
            compiler_params=pltpu.CompilerParams(
                collective_id=0, has_side_effects=True, vmem_limit_bytes=48 * 1024 * 1024
            ),
        )(
            *(
                pltpu.with_memory_space_constraint(x, pltpu.HBM)
                for x in (
                    positions,
                    queries.reshape(tokens * heads, head_size),
                    keys.reshape(tokens * kv_heads, head_size),
                    values.reshape(tokens * kv_heads, head_size),
                    jnp.asarray(table),
                )
            )
        )
        return out.reshape(tokens, heads, head_size)

    placed = (
        P(("groups", "ctx"), None, None),
        P(("groups", "ctx"), None, None),
        P(("groups", "ctx"), None, None),
        P(("groups", "ctx")),
    )
    return jax.shard_map(
        shards,
        mesh=mesh,
        in_specs=placed,
        out_specs=P(("groups", "ctx"), None, None),
        check_vma=False,
    )
```

```python
import functools
import math

import jax
import jax.numpy as jnp
import numpy as np
from jax import lax
from jax.experimental import pallas as pl
from jax.experimental.pallas import tpu as pltpu
from jax.sharding import PartitionSpec as P

TILE = 32
DOWN, UP = 0, 1
FAR = 3


def rotary_tables(tokens, head_size, stride):
    half = head_size // 2
    inverse = 1000000.0 ** (-2.0 * np.arange(half) / head_size)
    wide = lambda x: np.concatenate([x, x], -1)
    steps = (stride * np.arange(tokens))[:, None] * inverse[None, :]
    starts = np.arange(stride)[:, None] * inverse[None, :]
    return np.concatenate(
        [wide(np.cos(steps)), wide(np.sin(steps)), wide(np.cos(starts)), wide(np.sin(starts))]
    ).astype(np.float32)


def attend(
    n, kv_heads, per_group, tokens,
    place_hbm, q_hbm, k_hbm, v_hbm, table_hbm, out_ref,
    kv, kv_stage, q_all, q_stage, o_all, o_stage, offs, wide, small, m_ref, l_ref, acc_ref,
    place_ref, q_ref, k_ref, v_ref, table_ref,
    kv_recv, z_send, far_send, off_recv, offz_send, offfar_send, in_recv, in_send, inoff_recv, inoff_send,
    q_recv, q_send, o_recv, o_send, load_sem,
):
    loads = [
        pltpu.make_async_copy(src, dst, load_sem.at[i])
        for i, (src, dst) in enumerate(
            [(place_hbm, place_ref), (table_hbm, table_ref), (k_hbm, k_ref), (v_hbm, v_ref), (q_hbm, q_ref)]
        )
    ]
    for load in loads:
        load.start()
    head_size = q_ref.shape[-1]
    heads = kv_heads * per_group
    quartet = kv_heads
    rows = n // quartet
    pieces = tokens // TILE
    lanes = 2 * per_group * TILE
    factor = math.log2(math.e) / math.sqrt(head_size)
    me = lax.axis_index("ctx")
    z = me // quartet
    h = me % quartet
    column = h // 2
    core = h % 2
    mate = column * 2 + 1 - core
    across = (1 - column) * 2 + core
    diagonal = (1 - column) * 2 + 1 - core
    base = z * quartet

    def target(way, step):
        return me - step * quartet if way == DOWN else me + step * quartet

    def reaches(way, step):
        return z >= step if way == DOWN else z + step < rows

    barrier = pltpu.get_barrier_semaphore()

    def greet(peer):
        pl.semaphore_signal(barrier, inc=1, device_id={"ctx": peer})

    for peer in (mate, across, diagonal):
        greet(base + peer)
    greeted = 3
    for way in (DOWN, UP):
        for step in (1, FAR):
            greeted += reaches(way, step).astype(jnp.int32)

            @pl.when(reaches(way, step))
            def _():
                greet(target(way, step))

    def remote(src, dst, send_sem, recv_sem, target):
        return pltpu.make_async_remote_copy(
            src_ref=src, dst_ref=dst, send_sem=send_sem, recv_sem=recv_sem, device_id={"ctx": target}
        )

    def piece(way, row, p, half, first=None, count=2):
        first = 2 * half if first is None else first
        part = kv.at[row, p, pl.ds(first, count)]
        return remote(part, part, z_send.at[way, row, p, half], kv_recv.at[row, p, half], target(way, 1))

    def mark(way, row, first=0, count=quartet):
        part = offs.at[row, pl.ds(first, count)]
        return remote(part, part, offz_send.at[way, row], off_recv.at[row], target(way, 1))

    def far_piece(way, p, half, first=None, count=2):
        first = 2 * half if first is None else first
        part = kv.at[z, p, pl.ds(first, count)]
        return remote(part, part, far_send.at[way, p, half], kv_recv.at[z, p, half], target(way, FAR))

    def far_mark(way, first=0, count=quartet):
        part = offs.at[z, pl.ds(first, count)]
        return remote(part, part, offfar_send.at[way], off_recv.at[z], target(way, FAR))

    def near(p, src, dst):
        return remote(kv_stage.at[dst, p], kv.at[z, p, src], in_send.at[p, dst], in_recv.at[p, src], base + dst)

    def near_mark(src, dst):
        part = offs.at[z, src]
        return remote(part, part, inoff_send.at[dst], inoff_recv.at[src], base + dst)

    def near_q(src, dst):
        return remote(
            q_stage.at[dst], q_all.at[:, src // 2, src % 2], q_send.at[dst], q_recv.at[src], base + dst
        )

    def back(p, src, dst):
        return remote(o_stage.at[p, dst], o_all.at[p, src], o_send.at[p, dst], o_recv.at[p, src], base + dst)

    for load in loads[:2]:
        load.wait()
    offset = place_ref[0]
    c0 = table_ref[pl.ds(2 * tokens + offset, 1), :]
    s0 = table_ref[pl.ds(2 * tokens + n + offset, 1), :]
    ct, st = table_ref[:tokens, :], table_ref[tokens : 2 * tokens, :]
    lane = lax.broadcasted_iota(jnp.int32, (tokens, head_size), 1)
    cosine = ct * c0 - st * s0
    sine = st * c0 + ct * s0
    sine = jnp.where(lane < head_size // 2, -sine, sine)

    def rotated(x):
        return (x * cosine + pltpu.roll(x, head_size // 2, 1) * sine).astype(jnp.bfloat16)

    offs[z, h] = jnp.full((1, head_size), offset.astype(jnp.float32), jnp.float32)
    for load in loads[2:4]:
        load.wait()
    small[0] = k_ref[...].astype(jnp.float32)
    small[1] = v_ref[...].astype(jnp.float32)
    for k in range(kv_heads):
        x = rotated(small[0, pl.ds(k, tokens, stride=kv_heads), :])
        kv_stage[k, :, 0] = x.reshape(pieces, TILE, head_size)
        x = small[1, pl.ds(k, tokens, stride=kv_heads), :].astype(jnp.bfloat16)
        kv_stage[k, :, 1] = x.reshape(pieces, TILE, head_size)
    for p in range(pieces):
        kv[z, p, h] = kv_stage[h, p]

    pl.semaphore_wait(barrier, greeted)

    def spread(src, which, marks):
        for way in (DOWN, UP):

            @pl.when(reaches(way, FAR))
            def _():
                if marks:
                    far_mark(way, src, 1).start()
                for p in which:
                    far_piece(way, p, src // 2, src, 1).start()

            @pl.when(reaches(way, 1))
            def _():
                if marks:
                    mark(way, z, src, 1).start()
                for p in which:
                    piece(way, z, p, src // 2, src, 1).start()

    for dst in (across, diagonal, mate):
        near_mark(h, dst).start()
    for p in range(pieces):
        for dst in (across, diagonal, mate):
            near(p, h, dst).start()
    spread(h, range(pieces), True)

    loads[4].wait()
    wide[...] = q_ref[...].astype(jnp.float32)
    for k in range(kv_heads):
        for g in range(per_group):
            q = rotated(wide[pl.ds(k * per_group + g, tokens, stride=heads), :])
            q_stage[k, :, g] = q.reshape(pieces, TILE, head_size)
    for dst in (across, diagonal, mate):
        near_q(h, dst).start()
    q_all[:, column, core] = q_stage[h]

    near_mark(mate, h).wait_recv()
    for p in range(pieces):
        near(p, mate, h).wait_recv()
    spread(mate, range(pieces), True)

    m_ref[...] = jnp.full(m_ref.shape, -jnp.inf, jnp.float32)
    l_ref[...] = jnp.zeros(l_ref.shape, jnp.float32)
    acc_ref[...] = jnp.zeros(acc_ref.shape, jnp.float32)

    for p in range(pieces):
        for src in (across, diagonal):
            if p == 0:
                near_mark(src, h).wait_recv()
            near(p, src, h).wait_recv()
            spread(src, [p], p == 0)

    keys_tile = quartet * TILE
    key_at = (lax.broadcasted_iota(jnp.int32, (keys_tile, lanes), 0) % TILE * n).astype(jnp.float32)
    query_at = (lax.broadcasted_iota(jnp.int32, (1, lanes), 1) % TILE * n).astype(jnp.float32)

    def attention(cols, row, p):
        keys = kv[row, p, :, 0].reshape(keys_tile, head_size)
        values = kv[row, p, :, 1].reshape(keys_tile, head_size)
        blocks = [(i, col) for i in range(p, pieces) for col in cols]
        q = jnp.concatenate([q_all[i, col].reshape(lanes, head_size) for i, col in blocks], 0)
        scores = lax.dot_general(keys, q, (((1,), (1,)), ((), ())), preferred_element_type=jnp.float32)
        theirs = jnp.concatenate(
            [
                jnp.broadcast_to(jnp.concatenate([offs[row, i]] * (lanes // head_size), 1), (TILE, lanes))
                for i in range(quartet)
            ],
            0,
        )
        key_place = key_at + theirs
        weights, shrinks = [], []
        for at, (i, col) in enumerate(blocks):
            s = scores[:, at * lanes : (at + 1) * lanes]
            if i == p:
                ours = jnp.concatenate(
                    [jnp.concatenate([offs[z, 2 * col + c]] * (lanes // 2 // head_size), 1) for c in range(2)], 1
                )
                s = jnp.where(key_place <= query_at + ours, s, -jnp.inf)
            old = m_ref[i, col]
            top = jnp.maximum(old, jnp.max(s, axis=0, keepdims=True))
            shrink = jnp.exp2((old - top) * factor)
            w = jnp.exp2((s - top) * factor)
            m_ref[i, col] = top
            l_ref[i, col] = l_ref[i, col] * shrink + jnp.sum(w, axis=0, keepdims=True)
            weights.append(w.astype(jnp.bfloat16))
            shrinks.append(shrink)
        o = lax.dot_general(
            values, jnp.concatenate(weights, 1), (((0,), (0,)), ((), ())), preferred_element_type=jnp.float32
        )
        for at, (i, col) in enumerate(blocks):
            acc_ref[i, col] = acc_ref[i, col] * shrinks[at] + o[:, at * lanes : (at + 1) * lanes]

    def relayed(way, d):
        return reaches(way, 1) & ((d == 1) | (d >= FAR))

    def arrive(way, row, p):
        if p == 0:
            mark(way, row).wait_recv()
        for half in (column, 1 - column):
            piece(way, row, p, half).wait_recv()

    def each(d, do):
        for way in (DOWN, UP):
            row = z + d if way == DOWN else z - d

            @pl.when((row < rows) if way == DOWN else (row >= 0))
            def _():
                do(way, row)

    def relay(d, p):
        def do(way, row):
            @pl.when(relayed(way, d))
            def _():
                if p == 0:
                    mark(way, row).wait_recv()
                    mark(way, row).start()
                for half in (column, 1 - column):
                    piece(way, row, p, half).wait_recv()
                    piece(way, row, p, half).start()

        each(d, do)

    def take(d, p):
        def do(way, row):
            @pl.when(jnp.logical_not(relayed(way, d)))
            def _():
                arrive(way, row, p)

            attention((0, 1), row, p)

        each(d, do)

    def finish(p):
        for col in range(2):
            o = acc_ref[p, col] * (1.0 / l_ref[p, col])
            o = o.T.astype(jnp.bfloat16)
            for c in range(2):
                part = o[c * lanes // 2 : (c + 1) * lanes // 2]
                o_stage[p, 2 * col + c] = part.reshape(per_group, TILE, head_size)
        for dst in (across, diagonal, mate):
            back(p, h, dst).start()
        o_all[p, h] = o_stage[p, h]

    near_q(mate, h).wait_recv()
    for p in range(pieces):
        attention([column], z, p)
    relay(1, 0)
    relay(1, 1)
    for src in (across, diagonal):
        near_q(src, h).wait_recv()
    for p in range(pieces):
        attention([1 - column], z, p)
        if p == 0:
            for last in range(2, pieces):
                relay(1, last)

    if rows > FAR + 1:
        for p in range(pieces):
            relay(FAR, p)

        @pl.loop(FAR + 1, rows)
        def _(d):
            for p in range(pieces):
                relay(d, p)
                take(d, p)

    for p in range(pieces):
        for d in (1, 3, 2):
            take(d, p)
        finish(p)

    for p in range(pieces):
        for src in (across, diagonal, mate):
            back(p, src, h).wait_recv()
        for k in range(kv_heads):
            for g in range(per_group):
                at = p * TILE * heads + k * per_group + g
                wide[pl.ds(at, TILE, stride=heads), :] = o_all[p, k, g].astype(jnp.float32)
        span = slice(p * TILE * heads, (p + 1) * TILE * heads)
        out_ref[span, :] = wide[span, :].astype(jnp.bfloat16)

    for dst in (across, diagonal, mate):
        near_mark(h, dst).wait_send()
        near_q(h, dst).wait_send()
        for p in range(pieces):
            near(p, h, dst).wait_send()
            back(p, h, dst).wait_send()

    def sent(way, row, d):
        @pl.when(reaches(way, 1) if d is None else relayed(way, d))
        def _():
            mark(way, row).wait_send()
            for p in range(pieces):
                for half in range(2):
                    piece(way, row, p, half).wait_send()

    for way in (DOWN, UP):
        sent(way, z, None)

        @pl.when(reaches(way, FAR))
        def _():
            far_mark(way).wait_send()
            for p in range(pieces):
                for half in range(2):
                    far_piece(way, p, half).wait_send()

    @pl.loop(1, rows)
    def _(d):
        @pl.when(z + d < rows)
        def _():
            sent(DOWN, z + d, d)

        @pl.when(z - d >= 0)
        def _():
            sent(UP, z - d, d)


def solution(mesh):
    n = mesh.shape["ctx"]

    def shards(queries, keys, values, positions):
        tokens, heads, head_size = queries.shape
        kv_heads = keys.shape[1]
        per_group = heads // kv_heads
        table = rotary_tables(tokens, head_size, n)
        pieces = tokens // TILE
        rows = n // kv_heads
        lanes = 2 * per_group * TILE
        vmem = pl.BlockSpec(memory_space=pltpu.VMEM)
        hbm = pl.BlockSpec(memory_space=pl.ANY)
        dma = pltpu.SemaphoreType.DMA
        bf16, f32 = jnp.bfloat16, jnp.float32
        out = pl.pallas_call(
            functools.partial(attend, n, kv_heads, per_group, tokens),
            out_shape=jax.ShapeDtypeStruct((tokens * heads, head_size), bf16),
            in_specs=[hbm] * 5,
            out_specs=vmem,
            scratch_shapes=[
                pltpu.VMEM((rows, pieces, kv_heads, 2, TILE, head_size), bf16),
                pltpu.VMEM((kv_heads, pieces, 2, TILE, head_size), bf16),
                pltpu.VMEM((pieces, 2, 2, per_group, TILE, head_size), bf16),
                pltpu.VMEM((kv_heads, pieces, per_group, TILE, head_size), bf16),
                pltpu.VMEM((pieces, kv_heads, per_group, TILE, head_size), bf16),
                pltpu.VMEM((pieces, kv_heads, per_group, TILE, head_size), bf16),
                pltpu.VMEM((rows, kv_heads, 1, head_size), f32),
                pltpu.VMEM((tokens * heads, head_size), f32),
                pltpu.VMEM((2, tokens * kv_heads, head_size), f32),
                pltpu.VMEM((pieces, 2, 1, lanes), f32),
                pltpu.VMEM((pieces, 2, 1, lanes), f32),
                pltpu.VMEM((pieces, 2, head_size, lanes), f32),
                pltpu.SMEM((tokens,), jnp.int32),
                pltpu.VMEM((tokens * heads, head_size), bf16),
                pltpu.VMEM((tokens * kv_heads, head_size), bf16),
                pltpu.VMEM((tokens * kv_heads, head_size), bf16),
                pltpu.VMEM(table.shape, f32),
                dma((rows, pieces, 2)),
                dma((2, rows, pieces, 2)),
                dma((2, pieces, 2)),
                dma((rows,)),
                dma((2, rows)),
                dma((2,)),
                dma((pieces, kv_heads)),
                dma((pieces, kv_heads)),
                dma((kv_heads,)),
                dma((kv_heads,)),
                dma((kv_heads,)),
                dma((kv_heads,)),
                dma((pieces, kv_heads)),
                dma((pieces, kv_heads)),
                dma((5,)),
            ],
            compiler_params=pltpu.CompilerParams(
                collective_id=0, has_side_effects=True, vmem_limit_bytes=48 * 1024 * 1024
            ),
        )(
            *(
                pltpu.with_memory_space_constraint(x, pltpu.HBM)
                for x in (
                    positions,
                    queries.reshape(tokens * heads, head_size),
                    keys.reshape(tokens * kv_heads, head_size),
                    values.reshape(tokens * kv_heads, head_size),
                    jnp.asarray(table),
                )
            )
        )
        return out.reshape(tokens, heads, head_size)

    placed = (
        P(("groups", "ctx"), None, None),
        P(("groups", "ctx"), None, None),
        P(("groups", "ctx"), None, None),
        P(("groups", "ctx")),
    )
    return jax.shard_map(
        shards,
        mesh=mesh,
        in_specs=placed,
        out_specs=P(("groups", "ctx"), None, None),
        check_vma=False,
    )
```

```python
import functools
import math

import jax
import jax.numpy as jnp
import numpy as np
from jax import lax
from jax.experimental import pallas as pl
from jax.experimental.pallas import tpu as pltpu
from jax.sharding import PartitionSpec as P

UNIT = 16
DOWN, UP = 0, 1
FAR = 3


def rotary_tables(tokens, head_size, stride):
    half = head_size // 2
    inverse = 1000000.0 ** (-2.0 * np.arange(half) / head_size)
    wide = lambda x: np.concatenate([x, x], -1)
    steps = (stride * np.arange(tokens))[:, None] * inverse[None, :]
    starts = np.arange(stride)[:, None] * inverse[None, :]
    return np.concatenate(
        [wide(np.cos(steps)), wide(np.sin(steps)), wide(np.cos(starts)), wide(np.sin(starts))]
    ).astype(np.float32)


def cuts(units):
    whole = [(u, min(u + 2, units)) for u in range(0, units, 2)]
    last = whole[-1]
    return whole, whole[:-1] + [(u, u + 1) for u in range(*last)]


def attend(
    n, kv_heads, per_group, tokens,
    place_hbm, q_hbm, k_hbm, v_hbm, table_hbm, out_ref,
    kv, kv_stage, q_all, q_stage, o_all, o_stage, offs, wide, small, m_ref, l_ref, acc_ref,
    place_ref, q_ref, k_ref, v_ref, table_ref,
    kv_recv, z_send, far_send, off_recv, offz_send, in_recv, in_send, inoff_recv, inoff_send,
    q_recv, q_send, o_recv, o_send, alive, load_sem,
):
    loads = [
        pltpu.make_async_copy(src, dst, load_sem.at[i])
        for i, (src, dst) in enumerate(
            [(place_hbm, place_ref), (table_hbm, table_ref), (k_hbm, k_ref), (v_hbm, v_ref), (q_hbm, q_ref)]
        )
    ]
    for load in loads:
        load.start()
    head_size = q_ref.shape[-1]
    heads = kv_heads * per_group
    quartet = kv_heads
    rows = n // quartet
    units = tokens // UNIT
    steps, pieces = cuts(units)
    lanes = 2 * per_group * UNIT
    factor = math.log2(math.e) / math.sqrt(head_size)
    me = lax.axis_index("ctx")
    z = me // quartet
    h = me % quartet
    column = h // 2
    core = h % 2
    mate = column * 2 + 1 - core
    across = (1 - column) * 2 + core
    diagonal = (1 - column) * 2 + 1 - core
    base = z * quartet

    def target(way, step):
        return me - step * quartet if way == DOWN else me + step * quartet

    def reaches(way, step):
        return z >= step if way == DOWN else z + step < rows

    barrier = pltpu.get_barrier_semaphore()

    def greet(peer):
        pl.semaphore_signal(barrier, inc=1, device_id={"ctx": peer})

    for peer in (mate, across, diagonal):
        greet(base + peer)
    greeted = 3 + reaches(DOWN, FAR).astype(jnp.int32)
    for way in (DOWN, UP):
        greeted += reaches(way, 1).astype(jnp.int32)

        @pl.when(reaches(way, 1))
        def _():
            greet(target(way, 1))

    @pl.when(reaches(UP, FAR))
    def _():
        greet(target(UP, FAR))

    def remote(src, dst, send_sem, recv_sem, target):
        return pltpu.make_async_remote_copy(
            src_ref=src, dst_ref=dst, send_sem=send_sem, recv_sem=recv_sem, device_id={"ctx": target}
        )

    def part_of(row, i, first, count):
        u0, u1 = pieces[i]
        return kv.at[row, pl.ds(u0, u1 - u0), pl.ds(first, count)]

    def slot(row):
        d = jnp.abs(row - z)
        return jnp.where(d > 1, d - 1, d)

    def piece(way, row, i, half, first=None, count=2):
        part = part_of(row, i, 2 * half if first is None else first, count)
        return remote(part, part, z_send.at[way, slot(row)], kv_recv.at[row, i, half], target(way, 1))

    def far_piece(way, i, half, first=None, count=2):
        part = part_of(z, i, 2 * half if first is None else first, count)
        return remote(part, part, far_send.at[way], kv_recv.at[z, i, half], target(way, FAR))

    def mark(way, row, first=0, count=quartet):
        part = offs.at[row, pl.ds(first, count)]
        return remote(part, part, offz_send.at[way, slot(row)], off_recv.at[row], target(way, 1))

    def far_mark(way, first=0, count=quartet):
        part = offs.at[z, pl.ds(first, count)]
        return remote(part, part, far_send.at[2 + way], off_recv.at[z], target(way, FAR))

    def near(i, src, dst):
        u0, u1 = pieces[i]
        span = pl.ds(u0, u1 - u0)
        return remote(kv_stage.at[dst, span], kv.at[z, span, src], in_send, in_recv.at[i], base + dst)

    def near_whole(src, dst):
        return remote(kv_stage.at[dst], kv.at[z, :, src], in_send, in_recv.at[len(pieces)], base + dst)

    def near_mark(src, dst, mine):
        part = offs.at[z, src]
        return remote(part, part, inoff_send, inoff_recv.at[mine], base + dst)

    def near_q(src, dst, mine):
        return remote(q_stage.at[dst], q_all.at[:, src // 2, src % 2], q_send, q_recv.at[mine], base + dst)

    def back(i, src, dst):
        u0, u1 = pieces[i]
        span = pl.ds(u0, u1 - u0)
        return remote(o_stage.at[span, dst], o_all.at[span, src], o_send, o_recv.at[i], base + dst)

    def waits(ref, send=None, recv=None):
        copy = remote(ref, ref, in_send if send is None else send, in_send if recv is None else recv, me)
        copy.wait_send() if recv is None else copy.wait_recv()

    for load in loads[:2]:
        load.wait()
    offset = place_ref[0]
    c0 = table_ref[pl.ds(2 * tokens + offset, 1), :]
    s0 = table_ref[pl.ds(2 * tokens + n + offset, 1), :]
    ct, st = table_ref[:tokens, :], table_ref[tokens : 2 * tokens, :]
    lane = lax.broadcasted_iota(jnp.int32, (tokens, head_size), 1)
    cosine = ct * c0 - st * s0
    sine = st * c0 + ct * s0
    sine = jnp.where(lane < head_size // 2, -sine, sine)

    def rotated(x):
        return (x * cosine + pltpu.roll(x, head_size // 2, 1) * sine).astype(jnp.bfloat16)

    offs[z, h] = jnp.full((1, head_size), offset.astype(jnp.float32), jnp.float32)
    for load in loads[2:4]:
        load.wait()
    small[0] = k_ref[...].astype(jnp.float32)
    small[1] = v_ref[...].astype(jnp.float32)
    for k in range(kv_heads):
        x = rotated(small[0, pl.ds(k, tokens, stride=kv_heads), :])
        kv_stage[k, :, 0] = x.reshape(units, UNIT, head_size)
        x = small[1, pl.ds(k, tokens, stride=kv_heads), :].astype(jnp.bfloat16)
        kv_stage[k, :, 1] = x.reshape(units, UNIT, head_size)
    kv[z, :, h] = kv_stage[h]

    pl.semaphore_wait(barrier, greeted)

    @pl.when(reaches(DOWN, FAR))
    def _():
        pl.semaphore_signal(alive, inc=1, device_id={"ctx": target(DOWN, FAR)})

    def spread(which, half, first, count, marks):
        @pl.when(reaches(DOWN, FAR))
        def _():
            if marks:
                far_mark(DOWN, first, count).start()
            for i in which:
                far_piece(DOWN, i, half, first, count).start()

        for way in (DOWN, UP):

            @pl.when(reaches(way, 1))
            def _():
                if marks:
                    mark(way, z, first, count).start()
                for i in which:
                    piece(way, z, i, half, first, count).start()

    every = range(len(pieces))
    for dst in (across, diagonal):
        near_mark(h, dst, 0).start()
    for i in every:
        for dst in (across, diagonal):
            near(i, h, dst).start()
    near_mark(h, mate, 1).start()
    near_whole(h, mate).start()
    spread(every, column, h, 1, True)

    loads[4].wait()
    wide[...] = q_ref[...].astype(jnp.float32)
    for k in range(kv_heads):
        for g in range(per_group):
            q = rotated(wide[pl.ds(k * per_group + g, tokens, stride=heads), :])
            q_stage[k, :, g] = q.reshape(units, UNIT, head_size)
    for dst in (across, diagonal):
        near_q(h, dst, 0).start()
    near_q(h, mate, 1).start()
    q_all[:, column, core] = q_stage[h]

    near_mark(mate, h, 1).wait_recv()
    near_whole(mate, h).wait_recv()
    spread(every, column, mate, 1, True)

    other = 1 - column
    for i in every:
        if i == 0:
            waits(offs.at[z, pl.ds(2 * other, 2)], recv=inoff_recv.at[0])
        waits(part_of(z, i, 2 * other, 2), recv=in_recv.at[i])
        spread([i], other, 2 * other, 2, i == 0)

    @pl.when(reaches(UP, FAR))
    def _():
        pl.semaphore_wait(alive, 1)
        far_mark(UP).start()
        for i in every:
            for half in (column, other):
                far_piece(UP, i, half).start()

    query_at = (lax.broadcasted_iota(jnp.int32, (1, lanes), 1) % UNIT * n).astype(jnp.float32)
    first_core = lax.broadcasted_iota(jnp.int32, (1, lanes), 1) < lanes // 2

    def attention(cols, row, step, fresh=False):
        u0, u1 = step
        below, count = u0 * quartet * UNIT, u1 * quartet * UNIT
        keys = kv[row, :u1, :, 0].reshape(count, head_size)
        values = kv[row, :u1, :, 1].reshape(count, head_size)
        blocks = [(i, col) for i in range(u0, u1) for col in cols]
        q = jnp.concatenate([q_all[i, col].reshape(lanes, head_size) for i, col in blocks], 0)
        scores = lax.dot_general(keys, q, (((1,), (1,)), ((), ())), preferred_element_type=jnp.float32)
        key_at = lax.broadcasted_iota(jnp.int32, (UNIT, lanes), 0).astype(jnp.float32) * n
        theirs = [key_at + jnp.concatenate([offs[row, i]] * (lanes // head_size), 1) for i in range(quartet)]
        key_place = jnp.concatenate([x + u * UNIT * n for u in range(u0, u1) for x in theirs], 0)
        weights, shrinks = [], []
        for at, (i, col) in enumerate(blocks):
            s = scores[:, at * lanes : (at + 1) * lanes]
            ours = [jnp.concatenate([offs[z, 2 * col + c]] * (lanes // head_size), 1) for c in range(2)]
            query_place = query_at + i * UNIT * n + jnp.where(first_core, ours[0], ours[1])
            masked = jnp.where(key_place <= query_place, s[below:], -jnp.inf)
            s = jnp.concatenate([s[:below], masked], 0) if below else masked
            top = jnp.max(s, axis=0, keepdims=True)
            if not fresh:
                old = m_ref[i, col]
                top = jnp.maximum(old, top)
                shrink = jnp.exp2((old - top) * factor)
                shrinks.append(shrink)
            w = jnp.exp2((s - top) * factor)
            total = jnp.sum(w, axis=0, keepdims=True)
            m_ref[i, col] = top
            l_ref[i, col] = total if fresh else l_ref[i, col] * shrink + total
            weights.append(w.astype(jnp.bfloat16))
        o = lax.dot_general(
            values, jnp.concatenate(weights, 1), (((0,), (0,)), ((), ())), preferred_element_type=jnp.float32
        )
        for at, (i, col) in enumerate(blocks):
            part = o[:, at * lanes : (at + 1) * lanes]
            acc_ref[i, col] = part if fresh else acc_ref[i, col] * shrinks[at] + part

    def relayed(way, d):
        return reaches(way, 1) & ((d == 1) | (d >= FAR))

    def each(d, do):
        for way in (DOWN, UP):
            row = z + d if way == DOWN else z - d

            @pl.when((row < rows) if way == DOWN else (row >= 0))
            def _():
                do(way, row)

    def relay(d, i):
        def do(way, row):
            @pl.when(relayed(way, d))
            def _():
                if i == 0:
                    mark(way, row).wait_recv()
                    mark(way, row).start()
                for half in (column, other):
                    piece(way, row, i, half).wait_recv()
                    piece(way, row, i, half).start()

        each(d, do)

    def take(d, step):
        def do(way, row):
            @pl.when(jnp.logical_not(relayed(way, d)))
            def _():
                for i in every:
                    if step[0] <= pieces[i][0] < step[1]:
                        if i == 0:
                            mark(way, row).wait_recv()
                        for half in (column, other):
                            piece(way, row, i, half).wait_recv()

            attention((0, 1), row, step)

        each(d, do)

    def finish(i):
        for u in range(*pieces[i]):
            for col in range(2):
                o = acc_ref[u, col] * (1.0 / l_ref[u, col])
                o = o.T.astype(jnp.bfloat16)
                for c in range(2):
                    part = o[c * lanes // 2 : (c + 1) * lanes // 2]
                    o_stage[u, 2 * col + c] = part.reshape(per_group, UNIT, head_size)
        for dst in (across, diagonal, mate):
            back(i, h, dst).start()
        for u in range(*pieces[i]):
            o_all[u, h] = o_stage[u, h]

    near_q(mate, h, 1).wait_recv()
    for step in steps:
        attention([column], z, step, True)
    relay(1, 0)
    relay(1, 1)
    waits(q_all.at[:, other], recv=q_recv.at[0])
    for step in steps:
        attention([other], z, step, True)
        if step[0] == 0:
            for i in every[2:]:
                relay(1, i)

    if rows > FAR + 1:
        for i in every:
            relay(FAR, i)

        @pl.loop(FAR + 1, rows)
        def _(d):
            for i in every:
                relay(d, i)
            for step in steps:
                take(d, step)

    for step in steps:
        for d in (1, 3):
            take(d, step)
    for i in every:
        take(2, pieces[i])
        finish(i)

    for i in every:
        u0, u1 = pieces[i]
        waits(o_all.at[pl.ds(u0, u1 - u0), pl.ds(0, quartet - 1)], recv=o_recv.at[i])
        for u in range(u0, u1):
            for k in range(kv_heads):
                for g in range(per_group):
                    at = u * UNIT * heads + k * per_group + g
                    wide[pl.ds(at, UNIT, stride=heads), :] = o_all[u, k, g].astype(jnp.float32)
        span = slice(u0 * UNIT * heads, u1 * UNIT * heads)
        out_ref[span, :] = wide[span, :].astype(jnp.bfloat16)

    three = pl.ds(0, quartet - 1)
    waits(kv_stage.at[three], send=in_send)
    waits(offs.at[z, three], send=inoff_send)
    waits(q_stage.at[three], send=q_send)
    waits(o_stage.at[:, three], send=o_send)

    def sent(way, row):
        waits(offs.at[row], send=offz_send.at[way, slot(row)])
        waits(kv.at[row], send=z_send.at[way, slot(row)])

    for way in (DOWN, UP):

        @pl.when(reaches(way, 1))
        def _():
            sent(way, z)

        @pl.when(reaches(way, FAR))
        def _():
            waits(offs.at[z], send=far_send.at[2 + way])
            waits(kv.at[z], send=far_send.at[way])

    @pl.loop(1, rows)
    def _(d):
        @pl.when((z + d < rows) & relayed(DOWN, d))
        def _():
            sent(DOWN, z + d)

        @pl.when((z - d >= 0) & relayed(UP, d))
        def _():
            sent(UP, z - d)


def solution(mesh):
    n = mesh.shape["ctx"]

    def shards(queries, keys, values, positions):
        tokens, heads, head_size = queries.shape
        kv_heads = keys.shape[1]
        per_group = heads // kv_heads
        table = rotary_tables(tokens, head_size, n)
        units = tokens // UNIT
        pieces = len(cuts(units)[1])
        rows = n // kv_heads
        lanes = 2 * per_group * UNIT
        vmem = pl.BlockSpec(memory_space=pltpu.VMEM)
        hbm = pl.BlockSpec(memory_space=pl.ANY)
        dma = pltpu.SemaphoreType.DMA
        bf16, f32 = jnp.bfloat16, jnp.float32
        out = pl.pallas_call(
            functools.partial(attend, n, kv_heads, per_group, tokens),
            out_shape=jax.ShapeDtypeStruct((tokens * heads, head_size), bf16),
            in_specs=[hbm] * 5,
            out_specs=vmem,
            scratch_shapes=[
                pltpu.VMEM((rows, units, kv_heads, 2, UNIT, head_size), bf16),
                pltpu.VMEM((kv_heads, units, 2, UNIT, head_size), bf16),
                pltpu.VMEM((units, 2, 2, per_group, UNIT, head_size), bf16),
                pltpu.VMEM((kv_heads, units, per_group, UNIT, head_size), bf16),
                pltpu.VMEM((units, kv_heads, per_group, UNIT, head_size), bf16),
                pltpu.VMEM((units, kv_heads, per_group, UNIT, head_size), bf16),
                pltpu.VMEM((rows, kv_heads, 1, head_size), f32),
                pltpu.VMEM((tokens * heads, head_size), f32),
                pltpu.VMEM((2, tokens * kv_heads, head_size), f32),
                pltpu.VMEM((units, 2, 1, lanes), f32),
                pltpu.VMEM((units, 2, 1, lanes), f32),
                pltpu.VMEM((units, 2, head_size, lanes), f32),
                pltpu.SMEM((tokens,), jnp.int32),
                pltpu.VMEM((tokens * heads, head_size), bf16),
                pltpu.VMEM((tokens * kv_heads, head_size), bf16),
                pltpu.VMEM((tokens * kv_heads, head_size), bf16),
                pltpu.VMEM(table.shape, f32),
                dma((rows, pieces, 2)),
                dma((2, rows - 1)),
                dma((4,)),
                dma((rows,)),
                dma((2, rows - 1)),
                dma((pieces + 1,)),
                dma(()),
                dma((2,)),
                dma(()),
                dma((2,)),
                dma(()),
                dma((pieces,)),
                dma(()),
                pltpu.SemaphoreType.REGULAR,
                dma((5,)),
            ],
            compiler_params=pltpu.CompilerParams(
                collective_id=0, has_side_effects=True, vmem_limit_bytes=48 * 1024 * 1024
            ),
        )(
            *(
                pltpu.with_memory_space_constraint(x, pltpu.HBM)
                for x in (
                    positions,
                    queries.reshape(tokens * heads, head_size),
                    keys.reshape(tokens * kv_heads, head_size),
                    values.reshape(tokens * kv_heads, head_size),
                    jnp.asarray(table),
                )
            )
        )
        return out.reshape(tokens, heads, head_size)

    placed = (
        P(("groups", "ctx"), None, None),
        P(("groups", "ctx"), None, None),
        P(("groups", "ctx"), None, None),
        P(("groups", "ctx")),
    )
    return jax.shard_map(
        shards,
        mesh=mesh,
        in_specs=placed,
        out_specs=P(("groups", "ctx"), None, None),
        check_vma=False,
    )
```

```python
import functools
import math

import jax
import jax.numpy as jnp
import numpy as np
from jax import lax
from jax.experimental import pallas as pl
from jax.experimental.pallas import tpu as pltpu
from jax.sharding import PartitionSpec as P

UNIT = 16
DOWN, UP = 0, 1
FAR = 3


def rotary_tables(tokens, head_size, stride):
    half = head_size // 2
    inverse = 1000000.0 ** (-2.0 * np.arange(half) / head_size)
    wide = lambda x: np.concatenate([x, x], -1)
    steps = (stride * np.arange(tokens))[:, None] * inverse[None, :]
    starts = np.arange(stride)[:, None] * inverse[None, :]
    return np.concatenate(
        [wide(np.cos(steps)), wide(np.sin(steps)), wide(np.cos(starts)), wide(np.sin(starts))]
    ).astype(np.float32)


def cuts(units):
    whole = [(u, min(u + 2, units)) for u in range(0, units, 2)]
    last = whole[-1]
    return whole, whole[:-1] + [(u, u + 1) for u in range(*last)]


def attend(
    n, kv_heads, per_group, tokens,
    place_hbm, q_hbm, k_hbm, v_hbm, table_hbm, out_ref,
    kv, kv_stage, q_all, q_stage, o_all, o_stage, offs, wide, small, m_ref, l_ref, acc_ref,
    place_ref, q_ref, k_ref, v_ref, table_ref,
    kv_recv, z_send, far_send, off_recv, offz_send, in_recv, in_send, inoff_recv, inoff_send,
    q_recv, q_send, o_recv, o_send, alive, load_sem,
):
    loads = [
        pltpu.make_async_copy(src, dst, load_sem.at[i])
        for i, (src, dst) in enumerate(
            [(place_hbm, place_ref), (table_hbm, table_ref), (k_hbm, k_ref), (v_hbm, v_ref), (q_hbm, q_ref)]
        )
    ]
    for load in loads:
        load.start()
    head_size = q_ref.shape[-1]
    heads = kv_heads * per_group
    quartet = kv_heads
    rows = n // quartet
    units = tokens // UNIT
    steps, pieces = cuts(units)
    lanes = 2 * per_group * UNIT
    factor = math.log2(math.e) / math.sqrt(head_size)
    me = lax.axis_index("ctx")
    z = me // quartet
    h = me % quartet
    column = h // 2
    core = h % 2
    mate = column * 2 + 1 - core
    across = (1 - column) * 2 + core
    diagonal = (1 - column) * 2 + 1 - core
    base = z * quartet

    def target(way, step):
        return me - step * quartet if way == DOWN else me + step * quartet

    def reaches(way, step):
        return z >= step if way == DOWN else z + step < rows

    barrier = pltpu.get_barrier_semaphore()

    def greet(peer):
        pl.semaphore_signal(barrier, inc=1, device_id={"ctx": peer})

    for peer in (mate, across, diagonal):
        greet(base + peer)
    greeted = 3
    for step in (1, FAR):
        greeted += reaches(DOWN, step).astype(jnp.int32)

        @pl.when(reaches(UP, step))
        def _():
            greet(target(UP, step))

    def remote(src, dst, send_sem, recv_sem, target):
        return pltpu.make_async_remote_copy(
            src_ref=src, dst_ref=dst, send_sem=send_sem, recv_sem=recv_sem, device_id={"ctx": target}
        )

    def part_of(row, i, first, count):
        u0, u1 = pieces[i]
        return kv.at[row, pl.ds(u0, u1 - u0), pl.ds(first, count)]

    def slot(row):
        d = jnp.abs(row - z)
        return jnp.where(d > 1, d - 1, d)

    def piece(way, row, i, half, first=None, count=2):
        part = part_of(row, i, 2 * half if first is None else first, count)
        return remote(part, part, z_send.at[way, slot(row)], kv_recv.at[row, i, half], target(way, 1))

    def far_piece(way, i, half, first=None, count=2):
        part = part_of(z, i, 2 * half if first is None else first, count)
        return remote(part, part, far_send.at[way], kv_recv.at[z, i, half], target(way, FAR))

    def mark(way, row, first=0, count=quartet):
        part = offs.at[row, pl.ds(first, count)]
        return remote(part, part, offz_send.at[way, slot(row)], off_recv.at[row], target(way, 1))

    def far_mark(way, first=0, count=quartet):
        part = offs.at[z, pl.ds(first, count)]
        return remote(part, part, far_send.at[2 + way], off_recv.at[z], target(way, FAR))

    def near(i, src, dst):
        u0, u1 = pieces[i]
        span = pl.ds(u0, u1 - u0)
        return remote(kv_stage.at[dst, span], kv.at[z, span, src], in_send, in_recv.at[i], base + dst)

    def near_whole(src, dst):
        return remote(kv_stage.at[dst], kv.at[z, :, src], in_send, in_recv.at[len(pieces)], base + dst)

    def near_mark(src, dst, mine):
        part = offs.at[z, src]
        return remote(part, part, inoff_send, inoff_recv.at[mine], base + dst)

    def near_q(src, dst, mine):
        return remote(q_stage.at[dst], q_all.at[:, src // 2, src % 2], q_send, q_recv.at[mine], base + dst)

    def back(i, src, dst):
        u0, u1 = pieces[i]
        span = pl.ds(u0, u1 - u0)
        return remote(o_stage.at[span, dst], o_all.at[span, src], o_send, o_recv.at[i], base + dst)

    def waits(ref, send=None, recv=None):
        copy = remote(ref, ref, in_send if send is None else send, in_send if recv is None else recv, me)
        copy.wait_send() if recv is None else copy.wait_recv()

    for load in loads[:2]:
        load.wait()
    offset = place_ref[0]
    c0 = table_ref[pl.ds(2 * tokens + offset, 1), :]
    s0 = table_ref[pl.ds(2 * tokens + n + offset, 1), :]
    ct, st = table_ref[:tokens, :], table_ref[tokens : 2 * tokens, :]
    lane = lax.broadcasted_iota(jnp.int32, (tokens, head_size), 1)
    cosine = ct * c0 - st * s0
    sine = st * c0 + ct * s0
    sine = jnp.where(lane < head_size // 2, -sine, sine)

    def rotated(x):
        return (x * cosine + pltpu.roll(x, head_size // 2, 1) * sine).astype(jnp.bfloat16)

    offs[z, h] = jnp.full((1, head_size), offset.astype(jnp.float32), jnp.float32)
    for load in loads[2:4]:
        load.wait()
    small[0] = k_ref[...].astype(jnp.float32)
    small[1] = v_ref[...].astype(jnp.float32)
    for k in range(kv_heads):
        x = rotated(small[0, pl.ds(k, tokens, stride=kv_heads), :])
        kv_stage[k, :, 0] = x.reshape(units, UNIT, head_size)
        x = small[1, pl.ds(k, tokens, stride=kv_heads), :].astype(jnp.bfloat16)
        kv_stage[k, :, 1] = x.reshape(units, UNIT, head_size)
    kv[z, :, h] = kv_stage[h]

    pl.semaphore_wait(barrier, greeted)

    for at, step in enumerate((1, FAR)):

        @pl.when(reaches(DOWN, step))
        def _():
            pl.semaphore_signal(alive.at[at], inc=1, device_id={"ctx": target(DOWN, step)})

    def spread(way, which, half, first, count, marks):
        if way == DOWN:

            @pl.when(reaches(DOWN, FAR))
            def _():
                if marks:
                    far_mark(DOWN, first, count).start()
                for i in which:
                    far_piece(DOWN, i, half, first, count).start()

        @pl.when(reaches(way, 1))
        def _():
            if marks:
                mark(way, z, first, count).start()
            for i in which:
                piece(way, z, i, half, first, count).start()

    every = range(len(pieces))
    for dst in (across, diagonal):
        near_mark(h, dst, 0).start()
    for i in every:
        for dst in (across, diagonal):
            near(i, h, dst).start()
    near_mark(h, mate, 1).start()
    near_whole(h, mate).start()
    spread(DOWN, every, column, h, 1, True)

    loads[4].wait()
    wide[...] = q_ref[...].astype(jnp.float32)
    for k in range(kv_heads):
        for g in range(per_group):
            q = rotated(wide[pl.ds(k * per_group + g, tokens, stride=heads), :])
            q_stage[k, :, g] = q.reshape(units, UNIT, head_size)
    for dst in (across, diagonal):
        near_q(h, dst, 0).start()
    near_q(h, mate, 1).start()
    q_all[:, column, core] = q_stage[h]

    near_mark(mate, h, 1).wait_recv()
    near_whole(mate, h).wait_recv()
    spread(DOWN, every, column, mate, 1, True)

    @pl.when(reaches(UP, 1))
    def _():
        pl.semaphore_wait(alive.at[0], 1)

    spread(UP, every, column, 2 * column, 2, True)

    other = 1 - column
    for i in every:
        if i == 0:
            waits(offs.at[z, pl.ds(2 * other, 2)], recv=inoff_recv.at[0])
        waits(part_of(z, i, 2 * other, 2), recv=in_recv.at[i])
        for way in (DOWN, UP):
            spread(way, [i], other, 2 * other, 2, i == 0)

    @pl.when(reaches(UP, FAR))
    def _():
        pl.semaphore_wait(alive.at[1], 1)
        far_mark(UP).start()
        for i in every:
            for half in (column, other):
                far_piece(UP, i, half).start()

    query_at = (lax.broadcasted_iota(jnp.int32, (1, lanes), 1) % UNIT * n).astype(jnp.float32)
    first_core = lax.broadcasted_iota(jnp.int32, (1, lanes), 1) < lanes // 2

    def attention(cols, rows_in, step, span=None, fresh=False):
        u0, u1 = step
        k0, k1 = (0, u1) if span is None else span
        below = max(0, min(u0, k1) - k0) * quartet * UNIT
        count = (k1 - k0) * quartet * UNIT
        keys = jnp.concatenate([kv[row, k0:k1, :, 0].reshape(count, head_size) for row in rows_in], 0)
        values = jnp.concatenate([kv[row, k0:k1, :, 1].reshape(count, head_size) for row in rows_in], 0)
        blocks = [(i, col) for i in range(u0, u1) for col in cols]
        q = jnp.concatenate([q_all[i, col].reshape(lanes, head_size) for i, col in blocks], 0)
        scores = lax.dot_general(keys, q, (((1,), (1,)), ((), ())), preferred_element_type=jnp.float32)
        key_at = lax.broadcasted_iota(jnp.int32, (UNIT, lanes), 0).astype(jnp.float32) * n
        key_places = []
        for row in rows_in:
            theirs = [key_at + jnp.concatenate([offs[row, i]] * (lanes // head_size), 1) for i in range(quartet)]
            key_places.append(
                jnp.concatenate([x + u * UNIT * n for u in range(max(u0, k0), k1) for x in theirs], 0)
            )
        weights, shrinks = [], []
        for at, (i, col) in enumerate(blocks):
            s = scores[:, at * lanes : (at + 1) * lanes]
            ours = [jnp.concatenate([offs[z, 2 * col + c]] * (lanes // head_size), 1) for c in range(2)]
            query_place = query_at + i * UNIT * n + jnp.where(first_core, ours[0], ours[1])
            parts = []
            for r, key_place in enumerate(key_places):
                if below:
                    parts.append(s[r * count : r * count + below])
                late = s[r * count + below : (r + 1) * count]
                parts.append(jnp.where(key_place <= query_place, late, -jnp.inf))
            s = jnp.concatenate(parts, 0)
            top = jnp.max(s, axis=0, keepdims=True)
            if not fresh:
                old = m_ref[i, col]
                top = jnp.maximum(old, top)
                shrink = jnp.exp2((old - top) * factor)
                shrinks.append(shrink)
            w = jnp.exp2((s - top) * factor)
            total = jnp.sum(w, axis=0, keepdims=True)
            m_ref[i, col] = top
            l_ref[i, col] = total if fresh else l_ref[i, col] * shrink + total
            weights.append(w.astype(jnp.bfloat16))
        o = lax.dot_general(
            values, jnp.concatenate(weights, 1), (((0,), (0,)), ((), ())), preferred_element_type=jnp.float32
        )
        for at, (i, col) in enumerate(blocks):
            part = o[:, at * lanes : (at + 1) * lanes]
            acc_ref[i, col] = part if fresh else acc_ref[i, col] * shrinks[at] + part

    def relayed(way, d):
        return reaches(way, 1) & ((d == 1) | (d >= FAR))

    def each(d, do):
        for way in (DOWN, UP):
            row = z + d if way == DOWN else z - d

            @pl.when((row < rows) if way == DOWN else (row >= 0))
            def _():
                do(way, row)

    def relay(d, i):
        def do(way, row):
            @pl.when(relayed(way, d))
            def _():
                if i == 0:
                    mark(way, row).wait_recv()
                    mark(way, row).start()
                for half in (column, other):
                    piece(way, row, i, half).wait_recv()
                    piece(way, row, i, half).start()

        each(d, do)

    def come(d, step):
        def do(way, row):
            @pl.when(jnp.logical_not(relayed(way, d)))
            def _():
                for i in every:
                    if step[0] <= pieces[i][0] < step[1]:
                        if i == 0:
                            mark(way, row).wait_recv()
                        for half in (column, other):
                            piece(way, row, i, half).wait_recv()

        each(d, do)

    def take(d, step, queries=None, span=None):
        come(d, step)
        each(d, lambda way, row: attention((0, 1), [row], queries or step, span))

    def take_early(step):
        if rows == FAR + 1:
            come(1, step)
            come(FAR, step)
            attention((0, 1), [lax.rem(z + 1, rows), lax.rem(z + FAR, rows)], step)
        else:
            take(1, step)
            take(FAR, step)

    def finish(i):
        for u in range(*pieces[i]):
            for col in range(2):
                o = acc_ref[u, col] * (1.0 / l_ref[u, col])
                o = o.T.astype(jnp.bfloat16)
                for c in range(2):
                    part = o[c * lanes // 2 : (c + 1) * lanes // 2]
                    o_stage[u, 2 * col + c] = part.reshape(per_group, UNIT, head_size)
        for dst in (across, diagonal, mate):
            back(i, h, dst).start()
        for u in range(*pieces[i]):
            o_all[u, h] = o_stage[u, h]

    near_q(mate, h, 1).wait_recv()
    for step in steps:
        attention([column], [z], step, fresh=True)
    relay(1, 0)
    waits(q_all.at[:, other], recv=q_recv.at[0])
    for s, step in enumerate(steps):
        if s == len(steps) - 1:
            relay(1, 1)
        attention([other], [z], step, fresh=True)
    for i in every[2:]:
        relay(1, i)

    if rows > FAR + 1:
        for i in every:
            relay(FAR, i)

        @pl.loop(FAR + 1, rows)
        def _(d):
            for i in every:
                relay(d, i)
            for step in steps:
                take(d, step)

    ahead = 0
    for s, step in enumerate(steps):
        while ahead < min(s + 2, len(steps)):
            take_early(steps[ahead])
            ahead += 1
        if s < len(steps) - 1:
            take(2, step)
            finish(s)
    take(2, pieces[-2], steps[-1], (0, pieces[-2][1]))
    finish(len(pieces) - 2)
    take(2, pieces[-1], pieces[-1], pieces[-1])
    finish(len(pieces) - 1)

    for i in every:
        u0, u1 = pieces[i]
        waits(o_all.at[pl.ds(u0, u1 - u0), pl.ds(0, quartet - 1)], recv=o_recv.at[i])
        for u in range(u0, u1):
            for k in range(kv_heads):
                for g in range(per_group):
                    at = u * UNIT * heads + k * per_group + g
                    wide[pl.ds(at, UNIT, stride=heads), :] = o_all[u, k, g].astype(jnp.float32)
        span = slice(u0 * UNIT * heads, u1 * UNIT * heads)
        out_ref[span, :] = wide[span, :].astype(jnp.bfloat16)

    three = pl.ds(0, quartet - 1)
    waits(kv_stage.at[three], send=in_send)
    waits(offs.at[z, three], send=inoff_send)
    waits(q_stage.at[three], send=q_send)
    waits(o_stage.at[:, three], send=o_send)

    def sent(way, row):
        waits(offs.at[row], send=offz_send.at[way, slot(row)])
        waits(kv.at[row], send=z_send.at[way, slot(row)])

    for way in (DOWN, UP):

        @pl.when(reaches(way, 1))
        def _():
            sent(way, z)

        @pl.when(reaches(way, FAR))
        def _():
            waits(offs.at[z], send=far_send.at[2 + way])
            waits(kv.at[z], send=far_send.at[way])

    @pl.loop(1, rows)
    def _(d):
        @pl.when((z + d < rows) & relayed(DOWN, d))
        def _():
            sent(DOWN, z + d)

        @pl.when((z - d >= 0) & relayed(UP, d))
        def _():
            sent(UP, z - d)


def solution(mesh):
    n = mesh.shape["ctx"]

    def shards(queries, keys, values, positions):
        tokens, heads, head_size = queries.shape
        kv_heads = keys.shape[1]
        per_group = heads // kv_heads
        table = rotary_tables(tokens, head_size, n)
        units = tokens // UNIT
        pieces = len(cuts(units)[1])
        rows = n // kv_heads
        lanes = 2 * per_group * UNIT
        vmem = pl.BlockSpec(memory_space=pltpu.VMEM)
        hbm = pl.BlockSpec(memory_space=pl.ANY)
        dma = pltpu.SemaphoreType.DMA
        bf16, f32 = jnp.bfloat16, jnp.float32
        out = pl.pallas_call(
            functools.partial(attend, n, kv_heads, per_group, tokens),
            out_shape=jax.ShapeDtypeStruct((tokens * heads, head_size), bf16),
            in_specs=[hbm] * 5,
            out_specs=vmem,
            scratch_shapes=[
                pltpu.VMEM((rows, units, kv_heads, 2, UNIT, head_size), bf16),
                pltpu.VMEM((kv_heads, units, 2, UNIT, head_size), bf16),
                pltpu.VMEM((units, 2, 2, per_group, UNIT, head_size), bf16),
                pltpu.VMEM((kv_heads, units, per_group, UNIT, head_size), bf16),
                pltpu.VMEM((units, kv_heads, per_group, UNIT, head_size), bf16),
                pltpu.VMEM((units, kv_heads, per_group, UNIT, head_size), bf16),
                pltpu.VMEM((rows, kv_heads, 1, head_size), f32),
                pltpu.VMEM((tokens * heads, head_size), f32),
                pltpu.VMEM((2, tokens * kv_heads, head_size), f32),
                pltpu.VMEM((units, 2, 1, lanes), f32),
                pltpu.VMEM((units, 2, 1, lanes), f32),
                pltpu.VMEM((units, 2, head_size, lanes), f32),
                pltpu.SMEM((tokens,), jnp.int32),
                pltpu.VMEM((tokens * heads, head_size), bf16),
                pltpu.VMEM((tokens * kv_heads, head_size), bf16),
                pltpu.VMEM((tokens * kv_heads, head_size), bf16),
                pltpu.VMEM(table.shape, f32),
                dma((rows, pieces, 2)),
                dma((2, rows - 1)),
                dma((4,)),
                dma((rows,)),
                dma((2, rows - 1)),
                dma((pieces + 1,)),
                dma(()),
                dma((2,)),
                dma(()),
                dma((2,)),
                dma(()),
                dma((pieces,)),
                dma(()),
                pltpu.SemaphoreType.REGULAR((2,)),
                dma((5,)),
            ],
            compiler_params=pltpu.CompilerParams(
                collective_id=0, has_side_effects=True, vmem_limit_bytes=48 * 1024 * 1024
            ),
        )(
            *(
                pltpu.with_memory_space_constraint(x, pltpu.HBM)
                for x in (
                    positions,
                    queries.reshape(tokens * heads, head_size),
                    keys.reshape(tokens * kv_heads, head_size),
                    values.reshape(tokens * kv_heads, head_size),
                    jnp.asarray(table),
                )
            )
        )
        return out.reshape(tokens, heads, head_size)

    placed = (
        P(("groups", "ctx"), None, None),
        P(("groups", "ctx"), None, None),
        P(("groups", "ctx"), None, None),
        P(("groups", "ctx")),
    )
    return jax.shard_map(
        shards,
        mesh=mesh,
        in_specs=placed,
        out_specs=P(("groups", "ctx"), None, None),
        check_vma=False,
    )
```

```python
import functools
import math

import jax
import jax.numpy as jnp
import numpy as np
from jax import lax
from jax.experimental import pallas as pl
from jax.experimental.pallas import tpu as pltpu
from jax.sharding import PartitionSpec as P

UNIT = 16
CHUNKS = 3
DOWN, UP = 0, 1
FAR = 3


def rotary_tables(tokens, head_size, stride):
    half = head_size // 2
    inverse = 1000000.0 ** (-2.0 * np.arange(half) / head_size)
    wide = lambda x: np.concatenate([x, x], -1)
    steps = (stride * np.arange(tokens))[:, None] * inverse[None, :]
    starts = np.arange(stride)[:, None] * inverse[None, :]
    return np.concatenate(
        [wide(np.cos(steps)), wide(np.sin(steps)), wide(np.cos(starts)), wide(np.sin(starts))]
    ).astype(np.float32)


def cuts(units):
    whole = [(u, min(u + 2, units)) for u in range(0, units, 2)]
    last = whole[-1]
    return whole, whole[:-1] + [(u, u + 1) for u in range(*last)]


def attend(
    n, kv_heads, per_group, tokens,
    place_hbm, q_hbm, k_hbm, v_hbm, table_hbm, out_ref,
    kv, kv_stage, q_all, q_stage, o_all, o_stage, offs, wide, small, m_ref, l_ref, acc_ref,
    place_ref, q_ref, k_ref, v_ref, table_ref,
    kv_recv, z_send, far_send, off_recv, offz_send, in_recv, in_send, inoff_recv, inoff_send,
    q_recv, q_send, o_recv, o_send, alive, load_sem,
):
    loads = [
        pltpu.make_async_copy(src, dst, load_sem.at[i])
        for i, (src, dst) in enumerate(
            [(place_hbm, place_ref), (table_hbm, table_ref), (k_hbm, k_ref), (v_hbm, v_ref), (q_hbm, q_ref)]
        )
    ]
    for at, src, dst in ((2, k_hbm, k_ref), (3, v_hbm, v_ref), (1, table_hbm, table_ref)):
        size = src.shape[0] // CHUNKS // 8 * 8
        for c in range(CHUNKS):
            span = pl.ds(c * size, size if c < CHUNKS - 1 else src.shape[0] - c * size)
            pltpu.make_async_copy(src.at[span], dst.at[span], load_sem.at[at]).start()
    loads[0].start()
    head_size = q_ref.shape[-1]
    heads = kv_heads * per_group
    quartet = kv_heads
    rows = n // quartet
    units = tokens // UNIT
    steps, pieces = cuts(units)
    lanes = 2 * per_group * UNIT
    factor = math.log2(math.e) / math.sqrt(head_size)
    me = lax.axis_index("ctx")
    z = me // quartet
    h = me % quartet
    column = h // 2
    core = h % 2
    mate = column * 2 + 1 - core
    across = (1 - column) * 2 + core
    diagonal = (1 - column) * 2 + 1 - core
    base = z * quartet

    def target(way, step):
        return me - step * quartet if way == DOWN else me + step * quartet

    def reaches(way, step):
        return z >= step if way == DOWN else z + step < rows

    barrier = pltpu.get_barrier_semaphore()

    def greet(peer):
        pl.semaphore_signal(barrier, inc=1, device_id={"ctx": peer})

    for peer in (mate, across, diagonal):
        greet(base + peer)
    greeted = 3
    for step in (1, FAR):
        greeted += reaches(DOWN, step).astype(jnp.int32)

        @pl.when(reaches(UP, step))
        def _():
            greet(target(UP, step))

    def remote(src, dst, send_sem, recv_sem, target):
        return pltpu.make_async_remote_copy(
            src_ref=src, dst_ref=dst, send_sem=send_sem, recv_sem=recv_sem, device_id={"ctx": target}
        )

    mine = [(pieces[0], 0), ((pieces[0][1], units), 1)]
    others = [(span, 2 + i) for i, span in enumerate(pieces)]

    def part_of(row, item, first, count):
        (u0, u1), _ = item
        return kv.at[row, pl.ds(u0, u1 - u0), pl.ds(first, count)]

    def slot(row):
        d = jnp.abs(row - z)
        return jnp.where(d > 1, d - 1, d)

    def inbox(row, item, place):
        return kv_recv.at[lax.rem(row - place + rows, rows) - 1, item[1]]

    def mailbox(row, place):
        return off_recv.at[lax.rem(row - place + rows, rows) - 1]

    def reached(way, step):
        return z - step if way == DOWN else z + step

    def piece(way, row, item, half, first=None, count=2):
        part = part_of(row, item, 2 * half if first is None else first, count)
        return remote(part, part, z_send.at[way, slot(row)], inbox(row, item, reached(way, 1)), target(way, 1))

    def mark(way, row, first=0, count=quartet):
        part = offs.at[row, pl.ds(first, count)]
        return remote(part, part, offz_send.at[way, slot(row)], mailbox(row, reached(way, 1)), target(way, 1))

    def straight(way, item, half, first=None, count=2):
        part = part_of(z, item, 2 * half if first is None else first, count)
        return remote(part, part, far_send.at[way], inbox(z, item, reached(way, FAR)), target(way, FAR))

    def straight_mark(way, first=0, count=quartet):
        part = offs.at[z, pl.ds(first, count)]
        return remote(part, part, far_send.at[2 + way], mailbox(z, reached(way, FAR)), target(way, FAR))

    def got(row, item, half):
        waits(part_of(row, item, 2 * half, 2), recv=inbox(row, item, z))

    def got_mark(row):
        waits(offs.at[row], recv=mailbox(row, z))

    def near(i, src, dst):
        u0, u1 = pieces[i]
        span = pl.ds(u0, u1 - u0)
        return remote(kv_stage.at[dst, span], kv.at[z, span, src], in_send, in_recv.at[i], base + dst)

    def near_whole(src, dst):
        return remote(kv_stage.at[dst], kv.at[z, :, src], in_send, in_recv.at[len(pieces)], base + dst)

    def near_mark(src, dst, mine):
        part = offs.at[z, src]
        return remote(part, part, inoff_send, inoff_recv.at[mine], base + dst)

    def near_q(src, dst, mine):
        return remote(q_stage.at[dst], q_all.at[:, src // 2, src % 2], q_send, q_recv.at[mine], base + dst)

    def back(i, src, dst):
        u0, u1 = pieces[i]
        span = pl.ds(u0, u1 - u0)
        return remote(o_stage.at[span, dst], o_all.at[span, src], o_send, o_recv.at[i], base + dst)

    def waits(ref, send=None, recv=None):
        copy = remote(ref, ref, in_send if send is None else send, in_send if recv is None else recv, me)
        copy.wait_send() if recv is None else copy.wait_recv()

    for load in loads[:2]:
        load.wait()
    offset = place_ref[0]
    c0 = table_ref[pl.ds(2 * tokens + offset, 1), :]
    s0 = table_ref[pl.ds(2 * tokens + n + offset, 1), :]
    ct, st = table_ref[:tokens, :], table_ref[tokens : 2 * tokens, :]
    lane = lax.broadcasted_iota(jnp.int32, (tokens, head_size), 1)
    cosine = ct * c0 - st * s0
    sine = st * c0 + ct * s0
    sine = jnp.where(lane < head_size // 2, -sine, sine)

    def rotated(x):
        return (x * cosine + pltpu.roll(x, head_size // 2, 1) * sine).astype(jnp.bfloat16)

    offs[z, h] = jnp.full((1, head_size), offset.astype(jnp.float32), jnp.float32)
    for load in loads[2:4]:
        load.wait()
    loads[4].start()
    small[0] = k_ref[...].astype(jnp.float32)
    small[1] = v_ref[...].astype(jnp.float32)
    for k in range(kv_heads):
        x = rotated(small[0, pl.ds(k, tokens, stride=kv_heads), :])
        kv_stage[k, :, 0] = x.reshape(units, UNIT, head_size)
        x = small[1, pl.ds(k, tokens, stride=kv_heads), :].astype(jnp.bfloat16)
        kv_stage[k, :, 1] = x.reshape(units, UNIT, head_size)
    kv[z, :, h] = kv_stage[h]

    pl.semaphore_wait(barrier, greeted)

    for at, step in enumerate((1, FAR)):

        @pl.when(reaches(DOWN, step))
        def _():
            pl.semaphore_signal(alive.at[at], inc=1, device_id={"ctx": target(DOWN, step)})

    def spread(way, items, half, first, count, marks):
        if way == DOWN:

            @pl.when(reaches(DOWN, FAR))
            def _():
                if marks:
                    straight_mark(DOWN, first, count).start()
                for item in items:
                    straight(DOWN, item, half, first, count).start()

        @pl.when(reaches(way, 1))
        def _():
            if marks:
                mark(way, z, first, count).start()
            for item in items:
                piece(way, z, item, half, first, count).start()

    every = range(len(pieces))
    for dst in (across, diagonal):
        near_mark(h, dst, 0).start()
    for i in every:
        for dst in (across, diagonal):
            near(i, h, dst).start()
    near_mark(h, mate, 1).start()
    near_whole(h, mate).start()
    spread(DOWN, mine, column, h, 1, True)

    loads[4].wait()
    wide[...] = q_ref[...].astype(jnp.float32)
    for k in range(kv_heads):
        for g in range(per_group):
            q = rotated(wide[pl.ds(k * per_group + g, tokens, stride=heads), :])
            q_stage[k, :, g] = q.reshape(units, UNIT, head_size)
    for dst in (across, diagonal):
        near_q(h, dst, 0).start()
    near_q(h, mate, 1).start()
    q_all[:, column, core] = q_stage[h]

    near_mark(mate, h, 1).wait_recv()
    near_whole(mate, h).wait_recv()
    spread(DOWN, mine, column, mate, 1, True)

    @pl.when(reaches(UP, 1))
    def _():
        pl.semaphore_wait(alive.at[0], 1)

    spread(UP, mine, column, 2 * column, 2, True)

    other = 1 - column
    for i in every:
        if i == 0:
            waits(offs.at[z, pl.ds(2 * other, 2)], recv=inoff_recv.at[0])
        waits(part_of(z, others[i], 2 * other, 2), recv=in_recv.at[i])
        for way in (DOWN, UP):
            spread(way, [others[i]], other, 2 * other, 2, i == 0)

    @pl.when(reaches(UP, FAR))
    def _():
        pl.semaphore_wait(alive.at[1], 1)
        straight_mark(UP).start()
        for items, half in ((mine, column), (others, other)):
            for item in items:
                straight(UP, item, half).start()

    query_at = (lax.broadcasted_iota(jnp.int32, (1, lanes), 1) % UNIT * n).astype(jnp.float32)
    first_core = lax.broadcasted_iota(jnp.int32, (1, lanes), 1) < lanes // 2

    def attention(cols, rows_in, step, span=None, fresh=False):
        u0, u1 = step
        k0, k1 = (0, u1) if span is None else span
        below = max(0, min(u0, k1) - k0) * quartet * UNIT
        count = (k1 - k0) * quartet * UNIT
        keys = jnp.concatenate([kv[row, k0:k1, :, 0].reshape(count, head_size) for row in rows_in], 0)
        values = jnp.concatenate([kv[row, k0:k1, :, 1].reshape(count, head_size) for row in rows_in], 0)
        blocks = [(i, col) for i in range(u0, u1) for col in cols]
        q = jnp.concatenate([q_all[i, col].reshape(lanes, head_size) for i, col in blocks], 0)
        scores = lax.dot_general(keys, q, (((1,), (1,)), ((), ())), preferred_element_type=jnp.float32)
        key_at = lax.broadcasted_iota(jnp.int32, (UNIT, lanes), 0).astype(jnp.float32) * n
        key_places = []
        for row in rows_in:
            theirs = [key_at + jnp.concatenate([offs[row, i]] * (lanes // head_size), 1) for i in range(quartet)]
            key_places.append(
                jnp.concatenate([x + u * UNIT * n for u in range(max(u0, k0), k1) for x in theirs], 0)
            )
        weights, shrinks = [], []
        for at, (i, col) in enumerate(blocks):
            s = scores[:, at * lanes : (at + 1) * lanes]
            ours = [jnp.concatenate([offs[z, 2 * col + c]] * (lanes // head_size), 1) for c in range(2)]
            query_place = query_at + i * UNIT * n + jnp.where(first_core, ours[0], ours[1])
            parts = []
            for r, key_place in enumerate(key_places):
                if below:
                    parts.append(s[r * count : r * count + below])
                late = s[r * count + below : (r + 1) * count]
                parts.append(jnp.where(key_place <= query_place, late, -jnp.inf))
            s = jnp.concatenate(parts, 0)
            top = jnp.max(s, axis=0, keepdims=True)
            if not fresh:
                old = m_ref[i, col]
                top = jnp.maximum(old, top)
                shrink = jnp.exp2((old - top) * factor)
                shrinks.append(shrink)
            w = jnp.exp2((s - top) * factor)
            total = jnp.sum(w, axis=0, keepdims=True)
            m_ref[i, col] = top
            l_ref[i, col] = total if fresh else l_ref[i, col] * shrink + total
            weights.append(w.astype(jnp.bfloat16))
        o = lax.dot_general(
            values, jnp.concatenate(weights, 1), (((0,), (0,)), ((), ())), preferred_element_type=jnp.float32
        )
        for at, (i, col) in enumerate(blocks):
            part = o[:, at * lanes : (at + 1) * lanes]
            acc_ref[i, col] = part if fresh else acc_ref[i, col] * shrinks[at] + part

    def relayed(way, d):
        return reaches(way, 1) & ((d == 1) | (d >= FAR))

    def each(d, do):
        for way in (DOWN, UP):
            row = z + d if way == DOWN else z - d

            @pl.when((row < rows) if way == DOWN else (row >= 0))
            def _():
                do(way, row)

    def halves(i):
        return [(items[i], half) for items, half in ((mine, column), (others, other)) if i < len(items)]

    def relay(d, i):
        def do(way, row):
            @pl.when(relayed(way, d))
            def _():
                if i == 0:
                    got_mark(row)
                    mark(way, row).start()
                for item, half in halves(i):
                    got(row, item, half)
                    piece(way, row, item, half).start()

        each(d, do)

    def come(d, step):
        def do(way, row):
            @pl.when(jnp.logical_not(relayed(way, d)))
            def _():
                for i in every:
                    if step[0] <= pieces[i][0] < step[1]:
                        if i == 0:
                            got_mark(row)
                        for item, half in halves(i):
                            got(row, item, half)

        each(d, do)

    def take(d, step, queries=None, span=None):
        come(d, step)
        each(d, lambda way, row: attention((0, 1), [row], queries or step, span))

    def take_early(step):
        if rows == FAR + 1:
            come(1, step)
            come(FAR, step)
            attention((0, 1), [lax.rem(z + 1, rows), lax.rem(z + FAR, rows)], step)
        else:
            take(1, step)
            take(FAR, step)

    def finish(i):
        for u in range(*pieces[i]):
            for col in range(2):
                o = acc_ref[u, col] * (1.0 / l_ref[u, col])
                o = o.T.astype(jnp.bfloat16)
                for c in range(2):
                    part = o[c * lanes // 2 : (c + 1) * lanes // 2]
                    o_stage[u, 2 * col + c] = part.reshape(per_group, UNIT, head_size)
        for dst in (across, diagonal, mate):
            back(i, h, dst).start()
        for u in range(*pieces[i]):
            o_all[u, h] = o_stage[u, h]

    near_q(mate, h, 1).wait_recv()
    for step in steps:
        attention([column], [z], step, fresh=True)
    relay(1, 0)
    waits(q_all.at[:, other], recv=q_recv.at[0])
    for s, step in enumerate(steps):
        if s == len(steps) - 1:
            relay(1, 1)
        attention([other], [z], step, fresh=True)
    for i in every[2:]:
        relay(1, i)

    if rows > FAR + 1:
        for i in every:
            relay(FAR, i)

        @pl.loop(FAR + 1, rows)
        def _(d):
            for i in every:
                relay(d, i)
            for step in steps:
                take(d, step)

    ahead = 0
    for s, step in enumerate(steps):
        while ahead < min(s + 2, len(steps)):
            take_early(steps[ahead])
            ahead += 1
        if s < len(steps) - 1:
            take(2, step)
            finish(s)
    take(2, pieces[-2], steps[-1], (0, pieces[-2][1]))
    finish(len(pieces) - 2)
    take(2, pieces[-1], pieces[-1], pieces[-1])
    finish(len(pieces) - 1)

    three = pl.ds(0, quartet - 1)
    waits(kv_stage.at[three], send=in_send)
    waits(offs.at[z, three], send=inoff_send)
    waits(q_stage.at[three], send=q_send)

    def sent(way, row):
        waits(offs.at[row], send=offz_send.at[way, slot(row)])
        waits(kv.at[row], send=z_send.at[way, slot(row)])

    for way in (DOWN, UP):

        @pl.when(reaches(way, 1))
        def _():
            sent(way, z)

        @pl.when(reaches(way, FAR))
        def _():
            waits(offs.at[z], send=far_send.at[2 + way])
            waits(kv.at[z], send=far_send.at[way])

    @pl.loop(1, rows)
    def _(d):
        @pl.when((z + d < rows) & relayed(DOWN, d))
        def _():
            sent(DOWN, z + d)

        @pl.when((z - d >= 0) & relayed(UP, d))
        def _():
            sent(UP, z - d)

    for i in every:
        u0, u1 = pieces[i]
        waits(o_all.at[pl.ds(u0, u1 - u0), pl.ds(0, quartet - 1)], recv=o_recv.at[i])
        for u in range(u0, u1):
            for k in range(kv_heads):
                for g in range(per_group):
                    at = u * UNIT * heads + k * per_group + g
                    wide[pl.ds(at, UNIT, stride=heads), :] = o_all[u, k, g].astype(jnp.float32)
        span = slice(u0 * UNIT * heads, u1 * UNIT * heads)
        out_ref[span, :] = wide[span, :].astype(jnp.bfloat16)

    waits(o_stage.at[:, pl.ds(0, quartet - 1)], send=o_send)


def solution(mesh):
    n = mesh.shape["ctx"]

    def shards(queries, keys, values, positions):
        tokens, heads, head_size = queries.shape
        kv_heads = keys.shape[1]
        per_group = heads // kv_heads
        table = rotary_tables(tokens, head_size, n)
        units = tokens // UNIT
        pieces = len(cuts(units)[1])
        rows = n // kv_heads
        lanes = 2 * per_group * UNIT
        vmem = pl.BlockSpec(memory_space=pltpu.VMEM)
        hbm = pl.BlockSpec(memory_space=pl.ANY)
        dma = pltpu.SemaphoreType.DMA
        bf16, f32 = jnp.bfloat16, jnp.float32
        out = pl.pallas_call(
            functools.partial(attend, n, kv_heads, per_group, tokens),
            out_shape=jax.ShapeDtypeStruct((tokens * heads, head_size), bf16),
            in_specs=[hbm] * 5,
            out_specs=vmem,
            scratch_shapes=[
                pltpu.VMEM((rows, units, kv_heads, 2, UNIT, head_size), bf16),
                pltpu.VMEM((kv_heads, units, 2, UNIT, head_size), bf16),
                pltpu.VMEM((units, 2, 2, per_group, UNIT, head_size), bf16),
                pltpu.VMEM((kv_heads, units, per_group, UNIT, head_size), bf16),
                pltpu.VMEM((units, kv_heads, per_group, UNIT, head_size), bf16),
                pltpu.VMEM((units, kv_heads, per_group, UNIT, head_size), bf16),
                pltpu.VMEM((rows, kv_heads, 1, head_size), f32),
                pltpu.VMEM((tokens * heads, head_size), f32),
                pltpu.VMEM((2, tokens * kv_heads, head_size), f32),
                pltpu.VMEM((units, 2, 1, lanes), f32),
                pltpu.VMEM((units, 2, 1, lanes), f32),
                pltpu.VMEM((units, 2, head_size, lanes), f32),
                pltpu.SMEM((tokens,), jnp.int32),
                pltpu.VMEM((tokens * heads, head_size), bf16),
                pltpu.VMEM((tokens * kv_heads, head_size), bf16),
                pltpu.VMEM((tokens * kv_heads, head_size), bf16),
                pltpu.VMEM(table.shape, f32),
                dma((rows - 1, pieces + 2)),
                dma((2, max(2, rows - 2))),
                dma((4,)),
                dma((rows - 1,)),
                dma((2, max(2, rows - 2))),
                dma((pieces + 1,)),
                dma(()),
                dma((2,)),
                dma(()),
                dma((2,)),
                dma(()),
                dma((pieces,)),
                dma(()),
                pltpu.SemaphoreType.REGULAR((2,)),
                dma((5,)),
            ],
            compiler_params=pltpu.CompilerParams(
                collective_id=0, has_side_effects=True, vmem_limit_bytes=48 * 1024 * 1024
            ),
        )(
            *(
                pltpu.with_memory_space_constraint(x, pltpu.HBM)
                for x in (
                    positions,
                    queries.reshape(tokens * heads, head_size),
                    keys.reshape(tokens * kv_heads, head_size),
                    values.reshape(tokens * kv_heads, head_size),
                    jnp.asarray(table),
                )
            )
        )
        return out.reshape(tokens, heads, head_size)

    placed = (
        P(("groups", "ctx"), None, None),
        P(("groups", "ctx"), None, None),
        P(("groups", "ctx"), None, None),
        P(("groups", "ctx")),
    )
    return jax.shard_map(
        shards,
        mesh=mesh,
        in_specs=placed,
        out_specs=P(("groups", "ctx"), None, None),
        check_vma=False,
    )
```
